32 devices in a mesh: seq: 8 (over z, core), head: 2 (over x), dp: 2 (over y).
Axes of the slice: x: 2, y: 2, z: 4, core: 2. Of those that a mesh axis runs over, the one named last changes fastest.
Arguments:
- passthrough: bfloat16 [2, 2048, 1024], P('dp', 'seq', 'head'), may hold values from -6 to 6
- mixed_out: bfloat16 [2, 2048, 1024], P('dp', 'seq', 'head'), may hold values from -6 to 6
- grad_mixed: bfloat16 [2, 2048, 1024], P('dp', 'seq', 'head'), may hold values from -6 to 6
- grad_pass: bfloat16 [2, 2048, 1024], P('dp', 'seq', 'head'), may hold values from -6 to 6
- query_weight: bfloat16 [1024, 1024], P(None, 'head'), may hold values from -0.1875 to 0.1875
- key_weight: bfloat16 [1024, 1024], P(None, 'head'), may hold values from -0.1875 to 0.1875
- value_weight: bfloat16 [1024, 1024], P(None, 'head'), may hold values from -0.1875 to 0.1875
- random_features: bfloat16 [8, 128, 256], P('head'), may hold values from -5 to 5
- document_ids: int32 [2, 2048], P('dp', 'seq'), may hold values from 0 to 9, never falling along the last dimension, each value on 1 to 512 neighbouring positions
Outputs:
- first_in: bfloat16 [2, 2048, 1024], P('dp', 'seq', 'head')
- grad_second: bfloat16 [2, 2048, 1024], P('dp', 'seq', 'head')
- grad_query_weight: float32 [1024, 1024], P(('seq', 'dp'), 'head')
- grad_key_weight: float32 [1024, 1024], P(('seq', 'dp'), 'head')
- grad_value_weight: float32 [1024, 1024], P(('seq', 'dp'), 'head')
The draws below stay inside these ranges and needn't reach their ends.
Inputs may be any that keep to these rules, and one draw needn't show every extreme that they name: `document_ids`: along each context the number never falls; each of the 10 documents holds 1 to 512 positions, and one holds exactly 512.
All inputs are finite; a program needn't handle non-finite values.
Results may differ from the reference program's by a relative error of at most 0.018.
The reference program's roundings to bfloat16 on the way count: a program that leaves them out, or rounds other values in their place, can miss the bound.
Values may be sent and summed in bfloat16 or wider, within the bound.
No kernel may reach another device: no remote copies, remote signals or barrier semaphores. Data moves between devices by JAX's collectives and lax.ppermute only.
A program may use at most 64 MiB of HBM per device.

```python
import math
import jax
import jax.numpy as jnp
import numpy as np
from jax import lax

D = 1024
HEADS = 8
HD = 128
FEAT = 256
TOK_DEV = 256
SEQ = 2048
CTXS = 2
DOCS = 10
MOST = 512
N_SEQ = 8
N_HEAD = 2


def spiked(array, rng, source, target, shards_of, factor):
    def block_of(position):
        return (jnp.arange(array.shape[position]) // (array.shape[position] // shards_of)).reshape((-1,) + (1,) * (array.ndim - 1 - position))

    near = jax.random.permutation(rng, shards_of)[block_of(target)]
    far = (block_of(target) + shards_of // 2) % shards_of
    return jnp.where((block_of(source) == near) | (block_of(source) == far), factor * array, array)


def shard_levels(rng, extent, cuts, low, high):
    def one(dim, parts):
        draws = jax.random.uniform(jax.random.fold_in(jax.random.fold_in(rng, 6), dim), (parts,), jnp.float32, low / len(cuts), high / len(cuts))
        return jnp.repeat(jnp.exp(draws), extent[dim] // parts).reshape((-1,) + (1,) * (len(extent) - dim - 1))

    gain = one(*cuts[0])
    for cut in cuts[1:]:
        gain = gain * one(*cut)
    return gain


def split_up(number_of, total, most, skew):
    weights = [(1 << 20) // math.isqrt(rank ** skew) + 1 for rank in range(2, number_of + 1)]
    spare, counts = total - most - (number_of - 1), [1] * (number_of - 1)
    while spare > 0:
        movable = [i for i in range(number_of - 1) if counts[i] < most]
        whole, left = sum([weights[i] for i in movable]), spare
        for i in movable:
            more = min(most - counts[i], max(1, left * weights[i] // whole), spare)
            counts[i] = counts[i] + more
            spare = spare - more
    return np.array([most] + counts)


def ragged(own_key, amount, total, bound, slope):
    if amount == 2:
        one = jax.random.randint(own_key, (), max(1, total - bound), min(bound, total - 1) + 1)
        return jnp.stack([one, total - one])
    lengths = jnp.asarray(split_up(amount, total, bound, slope), jnp.int32)
    pairs = (amount - 1) // 2
    giver, taker = lengths[1:1 + 2 * pairs:2], lengths[2:2 + 2 * pairs:2]
    slack = jnp.minimum(giver - 1, bound - taker)
    moved = jax.random.randint(jax.random.fold_in(own_key, 1), (pairs,), 0, 1 << 20) % (slack + 1)
    lengths = lengths.at[1:1 + 2 * pairs:2].set(giver - moved).at[2:2 + 2 * pairs:2].set(taker + moved)
    return lengths[jax.random.permutation(jax.random.fold_in(own_key, 2), amount)]


def gaussian(key, dims, spread, bound, pieces=(), kind=jnp.bfloat16):
    array = jax.random.normal(key, dims, jnp.float32) * spread
    if len(pieces) > 0:
        array = shard_levels(key, dims, pieces, -0.22, 0.18) * array
    return jnp.clip(array, min=-bound, max=bound).astype(kind)


def heavy_noise(key, dims, scale, bound, pieces, heavy, held_as=jnp.bfloat16):
    array = scale * jax.random.normal(key, dims, jnp.float32)
    if pieces:
        array = array * shard_levels(key, dims, pieces, -0.22, 0.18)
    return jnp.clip(spiked(array, jax.random.fold_in(key, 3), *heavy), -bound, bound).astype(held_as)


def setup_inputs(seed: int = 0) -> dict:
    key_of = jax.random.split(jax.random.key(seed), 10)
    return {
        "passthrough": heavy_noise(key_of[0], (CTXS, SEQ, D), 1.0, 6.0, ((0, 2), (1, 8), (2, 2)), (1, 2, 8, 2.0)),
        "mixed_out": gaussian(key_of[1], (CTXS, SEQ, D), 1.0, 6.0, ((0, 2), (1, 8), (2, 2))),
        "grad_mixed": gaussian(key_of[2], (CTXS, SEQ, D), 1.0, 6.0, ((0, 2), (1, 8), (2, 2))),
        "grad_pass": gaussian(key_of[3], (CTXS, SEQ, D), 1.0, 6.0, ((0, 2), (1, 8), (2, 2))),
        "query_weight": gaussian(key_of[4], (D, D), D ** -0.5, 0.1875, ((1, 2),)),
        "key_weight": gaussian(key_of[5], (D, D), D ** -0.5, 0.1875, ((1, 2),)),
        "value_weight": gaussian(key_of[6], (D, D), D ** -0.5, 0.1875, ((1, 2),)),
        "random_features": gaussian(key_of[7], (HEADS, HD, FEAT), 1.0, 5.0, ((0, 2),)),
        "document_ids": jax.vmap(lambda own: jnp.searchsorted(jnp.cumsum(ragged(own, DOCS, SEQ, MOST, 2)), jnp.arange(SEQ), side="right"))(jax.random.split(key_of[8], CTXS)).reshape((CTXS, SEQ)).astype(jnp.int32),
    }


EPSILON = 1e-06
HIGHEST = lax.Precision.HIGHEST

def to_blocks(matrix):
    return matrix.reshape(N_SEQ, TOK_DEV, HEADS, HD).transpose(0, 2, 1, 3)

def from_blocks(tensor):
    return tensor.transpose(0, 2, 1, 3).reshape(N_SEQ * TOK_DEV, HEADS * HD)

def feature_map(projected, random_features):
    mixing = jnp.einsum('bhtd,hdm->bhtm', projected.astype(jnp.float32), random_features.astype(jnp.float32))
    widened = projected.astype(jnp.float32)
    squares = lax.optimization_barrier(jnp.sum(widened * widened, axis=-1, keepdims=True))
    exponent = mixing / HD ** 0.25 - squares / (2.0 * HD ** 0.5)
    return (jnp.exp(exponent) / FEAT ** 0.5).astype(jnp.bfloat16)

def feature_grad(dfeature, feature, projected, random_features):
    dexponent = dfeature * feature.astype(jnp.float32)
    rounded = dexponent.astype(jnp.bfloat16)
    back_proj = jnp.einsum('bhtm,hdm->bhtd', rounded.astype(jnp.float32), random_features.astype(jnp.float32))
    totals = lax.optimization_barrier(jnp.sum(dexponent, axis=-1, keepdims=True))
    result = back_proj / HD ** 0.25 - projected.astype(jnp.float32) * totals / HD ** 0.5
    return result.astype(jnp.bfloat16)

def carry_step(carry, element):
    state_in, state_id = carry
    block_state, block_id = element
    merged = block_state + jnp.where(state_id == block_id, state_in, jnp.zeros_like(state_in))
    return ((merged, block_id), carry)

def one_context(inputs, query_weight, key_weight, value_weight, random_features):
    passthrough, mixed_out, grad_mixed, grad_pass, doc_row = inputs
    widened = passthrough.astype(jnp.float32)
    inv_rms = lax.rsqrt(lax.optimization_barrier(jnp.mean(widened * widened, axis=-1, keepdims=True)) + EPSILON)
    norm_exact = widened * inv_rms
    normed = norm_exact.astype(jnp.bfloat16)
    query_all = jnp.dot(normed, query_weight, preferred_element_type=jnp.float32).astype(jnp.bfloat16)
    key_all = jnp.dot(normed, key_weight, preferred_element_type=jnp.float32).astype(jnp.bfloat16)
    value_all = jnp.dot(normed, value_weight, preferred_element_type=jnp.float32).astype(jnp.bfloat16)
    query_heads = to_blocks(query_all)
    key_heads = to_blocks(key_all)
    value_heads = to_blocks(value_all)
    feat_query = feature_map(query_heads, random_features)
    feat_key = feature_map(key_heads, random_features)
    fq_wide = feat_query.astype(jnp.float32)
    fk_wide = feat_key.astype(jnp.float32)
    value_wide = value_heads.astype(jnp.float32)
    block_ids = doc_row.reshape(N_SEQ, TOK_DEV).astype(jnp.int32)
    rows_idx = lax.broadcasted_iota(jnp.int32, (TOK_DEV, TOK_DEV), 0)
    cols_idx = lax.broadcasted_iota(jnp.int32, (TOK_DEV, TOK_DEV), 1)
    allowed = ((block_ids[:, :, None] == block_ids[:, None, :]) & (rows_idx >= cols_idx)[None])[:, None]
    scores = jnp.einsum('bhtm,bhsm->bhts', fq_wide, fk_wide)
    pair_weight = jnp.where(allowed, scores, 0.0).astype(jnp.bfloat16)
    pair_wide = pair_weight.astype(jnp.float32)
    attn_local = jnp.einsum('bhts,bhsd->bhtd', pair_wide, value_wide)
    last_ids = block_ids[:, -1]
    tail_mask = (block_ids == last_ids[:, None])[:, None, :, None]
    tail_state = jnp.einsum('bhtm,bhtd->bhmd', jnp.where(tail_mask, fk_wide, 0.0), value_wide)
    empty_state = jnp.zeros((HEADS, FEAT, HD), jnp.float32)
    _, (state_in, state_id) = lax.scan(carry_step, (empty_state, jnp.int32(-1)), (tail_state, last_ids))
    head_on = (block_ids == state_id[:, None])[:, None, :, None]
    carried = jnp.einsum('bhtm,bhmd->bhtd', fq_wide, state_in, precision=HIGHEST)
    attention = attn_local + jnp.where(head_on, carried, 0.0)
    inv_attn = lax.rsqrt(lax.optimization_barrier(jnp.mean(attention * attention, axis=-1, keepdims=True)) + EPSILON)
    act = attention * inv_attn
    first_in = (mixed_out.astype(jnp.float32) - from_blocks(act)).astype(jnp.bfloat16)
    grad_act = to_blocks(grad_mixed).astype(jnp.float32)
    grad_attn = (inv_attn * (grad_act - act * lax.optimization_barrier(jnp.mean(grad_act * act, axis=-1, keepdims=True)))).astype(jnp.bfloat16)
    grad_wide = grad_attn.astype(jnp.float32)
    dscores = jnp.einsum('bhtd,bhsd->bhts', grad_wide, value_wide)
    dpair = jnp.where(allowed, dscores, 0.0).astype(jnp.bfloat16).astype(jnp.float32)
    first_ids = block_ids[:, 0]
    head_mask = (block_ids == first_ids[:, None])[:, None, :, None]
    head_state = jnp.einsum('bhtm,bhtd->bhmd', jnp.where(head_mask, fq_wide, 0.0), grad_wide)
    _, (state_later, later_id) = lax.scan(carry_step, (empty_state, jnp.int32(-1)), (head_state, first_ids), reverse=True)
    tail_on = (block_ids == later_id[:, None])[:, None, :, None]
    dfeat_query = jnp.einsum('bhts,bhsm->bhtm', dpair, fk_wide)
    dfeat_query = dfeat_query + jnp.where(head_on, jnp.einsum('bhtd,bhmd->bhtm', grad_wide, state_in, precision=HIGHEST), 0.0)
    dfeat_key = jnp.einsum('bhts,bhtm->bhsm', dpair, fq_wide)
    dfeat_key = dfeat_key + jnp.where(tail_on, jnp.einsum('bhsd,bhmd->bhsm', value_wide, state_later, precision=HIGHEST), 0.0)
    dvalue = jnp.einsum('bhts,bhtd->bhsd', pair_wide, grad_wide)
    dvalue = (dvalue + jnp.where(tail_on, jnp.einsum('bhsm,bhmd->bhsd', fk_wide, state_later, precision=HIGHEST), 0.0)).astype(jnp.bfloat16)
    dquery = feature_grad(dfeat_query, feat_query, query_heads, random_features)
    dkey = feature_grad(dfeat_key, feat_key, key_heads, random_features)
    dquery_flat = from_blocks(dquery)
    dkey_flat = from_blocks(dkey)
    dvalue_flat = from_blocks(dvalue)
    group_width = D // N_HEAD
    grad_normed = jnp.zeros((N_SEQ * TOK_DEV, D), jnp.float32)
    for group in range(N_HEAD):
        low = group * group_width
        high = low + group_width
        term = jnp.dot(dquery_flat[:, low:high], query_weight[:, low:high].T, preferred_element_type=jnp.float32)
        term = term + jnp.dot(dkey_flat[:, low:high], key_weight[:, low:high].T, preferred_element_type=jnp.float32)
        term = term + jnp.dot(dvalue_flat[:, low:high], value_weight[:, low:high].T, preferred_element_type=jnp.float32)
        grad_normed = grad_normed + term.astype(jnp.bfloat16).astype(jnp.float32)
    dot_mean = lax.optimization_barrier(jnp.mean(grad_normed * norm_exact, axis=-1, keepdims=True))
    grad_second = (grad_pass.astype(jnp.float32) + inv_rms * (grad_normed - norm_exact * dot_mean)).astype(jnp.bfloat16)
    stacked = jnp.concatenate([dquery_flat, dkey_flat, dvalue_flat], axis=1)
    weight_term = jnp.dot(normed.T, stacked, preferred_element_type=jnp.float32)
    return (first_in, grad_second, weight_term)

def reference(passthrough, mixed_out, grad_mixed, grad_pass, query_weight, key_weight, value_weight, random_features, document_ids):

    def per_context(inputs):
        return one_context(inputs, query_weight, key_weight, value_weight, random_features)
    first_in, grad_second, weight_terms = lax.map(per_context, (passthrough, mixed_out, grad_mixed, grad_pass, document_ids))
    summed = lax.optimization_barrier(jnp.sum(weight_terms, axis=0)) / (CTXS * SEQ) ** 0.5
    return (first_in, grad_second, summed[:, :D], summed[:, D:2 * D], summed[:, 2 * D:])
```

```python
import jax
import jax.numpy as jnp
from jax import lax
from jax.experimental import pallas as pl
from jax.experimental.pallas import tpu as pltpu
from jax.sharding import PartitionSpec as P

EPSILON = 1e-06
F32 = jnp.float32
BF16 = jnp.bfloat16
PAD = 16


NN = (((1,), (0,)), ((), ()))
NT = (((1,), (1,)), ((), ()))
TN = (((0,), (0,)), ((), ()))


def mm(a, b, dims=NN):
    return lax.dot_general(a, b, dims, preferred_element_type=F32)


def call(name, body, outs, scalars, *arrays, flops=2e9, scratch=()):
    specs = [pl.BlockSpec(memory_space=pltpu.SMEM)] + [
        pl.BlockSpec(memory_space=pltpu.VMEM) for _ in arrays
    ]
    return pl.pallas_call(
        body,
        name=name,
        out_shape=[jax.ShapeDtypeStruct(s, d) for s, d in outs],
        in_specs=specs,
        out_specs=[pl.BlockSpec(memory_space=pltpu.VMEM) for _ in outs],
        scratch_shapes=list(scratch),
        cost_estimate=pl.CostEstimate(
            flops=int(flops),
            transcendentals=0,
            bytes_accessed=sum(a.size * a.dtype.itemsize for a in arrays),
        ),
    )(scalars, *arrays)


def features(projected, directions, head_dim, count):
    mixing = mm(projected, directions)
    wide = projected.astype(F32)
    squares = jnp.sum(wide * wide, axis=1, keepdims=True)
    exponent = mixing * (1.0 / head_dim**0.25) - squares * (1.0 / (2.0 * head_dim**0.5))
    return (jnp.exp(exponent) * (1.0 / count**0.5)).astype(BF16)


def features_back(dfeature, feature, projected, directions, head_dim):
    dexponent = dfeature * feature.astype(F32)
    back = mm(dexponent.astype(BF16), directions, NT)
    totals = jnp.sum(dexponent, axis=1, keepdims=True)
    result = back * (1.0 / head_dim**0.25) - projected.astype(F32) * (totals * (1.0 / head_dim**0.5))
    return result.astype(BF16)


def eye(n):
    return lax.broadcasted_iota(jnp.int32, (n, n), 0) == lax.broadcasted_iota(jnp.int32, (n, n), 1)


def row_to_col(row, n):
    return jnp.sum(jnp.where(eye(n), row, 0.0), axis=1, keepdims=True)


def col_to_row(col, n):
    return jnp.sum(jnp.where(eye(n), col, 0.0), axis=0, keepdims=True)


def pairs_allowed(id_col, id_row):
    n = id_row.shape[1]
    causal = lax.broadcasted_iota(jnp.int32, (n, n), 0) >= lax.broadcasted_iota(jnp.int32, (n, n), 1)
    return (id_col == id_row) & causal


def merged(refs, wanted, rows):
    total = None
    for ref in refs:
        number = ref[rows : rows + PAD, :].astype(F32)[0:1, 0:1]
        part = ref[0:rows, :].astype(F32) * (number == wanted).astype(F32)
        total = part if total is None else total + part
    return total.astype(BF16)


def shards(
    passthrough,
    mixed_out,
    grad_mixed,
    grad_pass,
    query_weight,
    key_weight,
    value_weight,
    random_features,
    document_ids,
):
    count_ctx, tok, width = passthrough.shape
    heads, head_dim, feats = random_features.shape
    assert count_ctx == 1 and heads * head_dim == width and tok <= width
    seq_count, head_count, dp_count = (lax.axis_size(a) for a in ("seq", "head", "dp"))
    seq_at, head_at, dp_at = (lax.axis_index(a) for a in ("seq", "head", "dp"))
    full = width * head_count
    pair_count = seq_count // 2
    assert seq_count % 2 == 0 and pair_count & (pair_count - 1) == 0
    total_rows = count_ctx * tok * seq_count * dp_count
    grad_scale = 1.0 / total_rows**0.5
    reach = max(1, -(-(seq_count * tok // 4 - 1) // tok))
    srows = heads * feats

    x_own = passthrough[0]
    x_others = [
        lax.ppermute(x_own, "head", [(j, (j - p) % head_count) for j in range(head_count)])
        for p in range(1, head_count)
    ]
    id_row = document_ids.astype(F32)
    scalars = jnp.concatenate(
        [
            document_ids[0, :1],
            document_ids[0, -1:],
            jnp.stack([(head_at + p) % head_count * width for p in range(head_count)]).astype(jnp.int32),
        ]
    )

    def hsl(h):
        return slice(h * head_dim, (h + 1) * head_dim)

    def fsl(h):
        return slice(h * feats, (h + 1) * feats)

    def keys_body(sc, ids, *refs):
        xs, (wk, wv, rf) = refs[:head_count], refs[head_count : head_count + 3]
        normed, inv_out, key, value, feat_key, tail, id_out = refs[head_count + 3 :]
        squares = None
        for x in xs:
            wide = x[...].astype(F32)
            part = jnp.sum(wide * wide, axis=1, keepdims=True)
            squares = part if squares is None else squares + part
        inv = lax.rsqrt(squares * (1.0 / full) + EPSILON)
        inv_out[...] = jnp.broadcast_to(inv, inv_out.shape)
        for p, x in enumerate(xs):
            at = pl.multiple_of(sc[2 + p], 128)
            normed[:, pl.ds(at, width)] = (x[...].astype(F32) * inv).astype(BF16)
        id_col = row_to_col(ids[...], tok)
        id_out[...] = jnp.broadcast_to(id_col, id_out.shape)
        n = normed[...]
        key[...] = mm(n, wk[...]).astype(BF16)
        value[...] = mm(n, wv[...]).astype(BF16)
        last = sc[1].astype(F32)
        on = id_col == last
        for h in range(heads):
            feat = features(key[:, hsl(h)], rf[h], head_dim, feats)
            feat_key[:, fsl(h)] = feat
            masked = jnp.where(on, feat.astype(F32), 0.0).astype(BF16)
            tail[fsl(h), :] = mm(masked, value[:, hsl(h)], TN).astype(BF16)
        tail[srows : srows + PAD, :] = jnp.full((PAD, head_dim), last, F32).astype(BF16)

    normed, inv_rms, key, value, feat_key, tail, id_col = call(
        "keys",
        keys_body,
        [
            ((tok, full), BF16),
            ((tok, 128), F32),
            ((tok, width), BF16),
            ((tok, width), BF16),
            ((tok, srows), BF16),
            ((srows + PAD, head_dim), BF16),
            ((tok, 128), F32),
        ],
        scalars,
        id_row,
        x_own,
        *x_others,
        key_weight,
        value_weight,
        random_features,
    )

    def shifted(state, sign):
        return [
            lax.ppermute(
                state,
                "seq",
                [(j, j + sign * k) for j in range(seq_count) if 0 <= j + sign * k < seq_count],
            )
            for k in range(1, reach + 1)
        ]

    earlier = shifted(tail, 1)

    def queries_body(sc, ids, idc, normed, wq, rf, feat_key, value, query, feat_query, pair, local):
        query[...] = mm(normed[...], wq[...]).astype(BF16)
        allowed = pairs_allowed(idc[:, 0:1], ids[...])
        for h in range(heads):
            feat = features(query[:, hsl(h)], rf[h], head_dim, feats)
            feat_query[:, fsl(h)] = feat
            scores = mm(feat, feat_key[:, fsl(h)], NT)
            weights = jnp.where(allowed, scores, 0.0).astype(BF16)
            pair[h] = weights
            local[:, hsl(h)] = mm(weights, value[:, hsl(h)])

    query, feat_query, pair, attn_local = call(
        "queries",
        queries_body,
        [
            ((tok, width), BF16),
            ((tok, srows), BF16),
            ((heads, tok, tok), BF16),
            ((tok, width), F32),
        ],
        scalars,
        id_row,
        id_col,
        normed,
        query_weight,
        random_features,
        feat_key,
        value,
    )

    pair_at, core_at = seq_at // 2, seq_at % 2
    blocks = pair_count * dp_count
    block_rows = full // (2 * blocks)

    def block_order(core):
        return [
            ((pair_at ^ k) * 2 + core) * dp_count + (dp_at + p) % dp_count
            for p in range(dp_count)
            for k in range(pair_count)
        ]

    order = jnp.stack(block_order(core_at) + block_order(1 - core_at)).astype(jnp.int32)

    def turned_body(sc, normed, mine, theirs, held):
        turned = normed[...].astype(F32).T
        for b in range(2 * blocks):
            held[b] = turned[b * block_rows : (b + 1) * block_rows, :].astype(BF16)
        for b in range(blocks):
            mine[b] = held[sc[b]]
            theirs[b] = held[sc[blocks + b]]

    shape3 = (blocks, block_rows, tok)
    mine_t, theirs_t = call(
        "turned",
        turned_body,
        [(shape3, BF16), (shape3, BF16)],
        order,
        normed,
        scratch=[pltpu.VMEM((2 * blocks, block_rows, tok), BF16)],
    )
    sibling = [(j, j ^ 1) for j in range(seq_count)]
    sibling_t = lax.ppermute(theirs_t, "seq", sibling)
    mine_t = mine_t.reshape(blocks * block_rows, tok)
    sibling_t = sibling_t.reshape(blocks * block_rows, tok)

    def attend_body(sc, idc, feat_query, local, mixed, gmixed, *refs):
        states, (first_in, grad_attn, head_state, state) = refs[:reach], refs[reach:]
        first = sc[0].astype(F32)
        state[...] = merged(states, first, srows)
        on = idc[:, 0:1] == first
        for h in range(heads):
            fq = feat_query[:, fsl(h)]
            carried = mm(fq, state[fsl(h), :])
            attn = local[:, hsl(h)] + jnp.where(on, carried, 0.0)
            inv = lax.rsqrt(jnp.mean(attn * attn, axis=1, keepdims=True) + EPSILON)
            act = attn * inv
            first_in[:, hsl(h)] = (mixed[:, hsl(h)].astype(F32) - act).astype(BF16)
            g = gmixed[:, hsl(h)].astype(F32)
            ga = (inv * (g - act * jnp.mean(g * act, axis=1, keepdims=True))).astype(BF16)
            grad_attn[:, hsl(h)] = ga
            masked = jnp.where(on, fq.astype(F32), 0.0).astype(BF16)
            head_state[fsl(h), :] = mm(masked, ga, TN).astype(BF16)
        head_state[srows : srows + PAD, :] = jnp.full((PAD, head_dim), first, F32).astype(BF16)

    first_in, grad_attn, head_state, state_in = call(
        "attend",
        attend_body,
        [
            ((tok, width), BF16),
            ((tok, width), BF16),
            ((srows + PAD, head_dim), BF16),
            ((srows, head_dim), BF16),
        ],
        scalars,
        id_col,
        feat_query,
        attn_local,
        mixed_out[0],
        grad_mixed[0],
        *earlier,
    )

    later = shifted(head_state, -1)

    def dquery_body(sc, ids, idc, grad_attn, value, feat_key, feat_query, query, rf, state, dquery, dpair):
        first = sc[0].astype(F32)
        on = idc[:, 0:1] == first
        allowed = pairs_allowed(idc[:, 0:1], ids[...])
        for h in range(heads):
            ga = grad_attn[:, hsl(h)]
            dscores = mm(ga, value[:, hsl(h)], NT)
            dp = jnp.where(allowed, dscores, 0.0).astype(BF16)
            dpair[h] = dp
            dfeat = mm(dp, feat_key[:, fsl(h)]) + jnp.where(on, mm(ga, state[fsl(h), :], NT), 0.0)
            dquery[:, hsl(h)] = features_back(
                dfeat, feat_query[:, fsl(h)], query[:, hsl(h)], rf[h], head_dim
            )

    dquery, dpair = call(
        "dquery",
        dquery_body,
        [((tok, width), BF16), ((heads, tok, tok), BF16)],
        scalars,
        id_row,
        id_col,
        grad_attn,
        value,
        feat_key,
        feat_query,
        query,
        random_features,
        state_in,
    )
    dquery_sib = lax.ppermute(dquery, "seq", sibling)

    def local_body(sc, dpair, pair, feat_query, grad_attn, dfeat, dvalue):
        for h in range(heads):
            dfeat[:, fsl(h)] = mm(dpair[h], feat_query[:, fsl(h)], TN)
            dvalue[:, hsl(h)] = mm(pair[h], grad_attn[:, hsl(h)], TN)

    dfeat_local, dvalue_local = call(
        "local",
        local_body,
        [((tok, srows), F32), ((tok, width), F32)],
        scalars,
        dpair,
        pair,
        feat_query,
        grad_attn,
    )

    rows_send = pair_count * block_rows

    def weight_body(sc, mine, sib, d, dsib, keep, *sends):
        for p in range(dp_count):
            at = slice(p * rows_send, (p + 1) * rows_send)
            part = (mm(mine[at, :], d[...]) + mm(sib[at, :], dsib[...])) * grad_scale
            if p == 0:
                keep[...] = part
            else:
                sends[p - 1][...] = part.astype(BF16)

    def weight_term(name, d, dsib):
        outs = call(
            name,
            weight_body,
            [((rows_send, width), F32)] + [((rows_send, width), BF16)] * (dp_count - 1),
            scalars,
            mine_t,
            sibling_t,
            d,
            dsib,
        )
        return outs[0], [
            lax.ppermute(o, "dp", [(j, (j + p) % dp_count) for j in range(dp_count)])
            for p, o in enumerate(outs[1:], 1)
        ]

    def rows_body(sc, keep, *refs):
        got, (own, *sends) = refs[: dp_count - 1], refs[dp_count - 1 :]
        for k in range(pair_count):
            at = slice(k * block_rows, (k + 1) * block_rows)
            total = keep[at, :]
            for g in got:
                total = total + g[at, :].astype(F32)
            if k == 0:
                own[...] = total
            else:
                sends[k - 1][...] = total.astype(BF16)

    def rows_term(name, keep, got):
        outs = call(
            name,
            rows_body,
            [((block_rows, width), F32)] + [((block_rows, width), BF16)] * (pair_count - 1),
            scalars,
            keep,
            *got,
        )
        return outs[0], [
            lax.ppermute(o, "seq", [(j, ((j // 2) ^ k) * 2 + j % 2) for j in range(seq_count)])
            for k, o in enumerate(outs[1:], 1)
        ]

    def final_term(own, got):
        for g in got:
            own = own + g.astype(F32)
        return own

    keep_q, got_q = weight_term("weight_q", dquery, dquery_sib)

    def dkeys_body(sc, idc, dfeat_local, dvalue_local, feat_key, value, key, rf, *refs):
        states, (dkey, dvalue) = refs[:reach], refs[reach : reach + 2]
        last = sc[1].astype(F32)
        state = merged(states, last, srows)
        on = idc[:, 0:1] == last
        for h in range(heads):
            fk = feat_key[:, fsl(h)]
            st = state[fsl(h), :]
            dvalue[:, hsl(h)] = (
                dvalue_local[:, hsl(h)] + jnp.where(on, mm(fk, st), 0.0)
            ).astype(BF16)
        for h in range(heads):
            fk = feat_key[:, fsl(h)]
            st = state[fsl(h), :]
            dfeat = dfeat_local[:, fsl(h)] + jnp.where(on, mm(value[:, hsl(h)], st, NT), 0.0)
            dkey[:, hsl(h)] = features_back(dfeat, fk, key[:, hsl(h)], rf[h], head_dim)

    dkey, dvalue = call(
        "dkeys",
        dkeys_body,
        [((tok, width), BF16), ((tok, width), BF16)],
        scalars,
        id_col,
        dfeat_local,
        dvalue_local,
        feat_key,
        value,
        key,
        random_features,
        *later,
    )
    dvalue_sib = lax.ppermute(dvalue, "seq", sibling)
    dkey_sib = lax.ppermute(dkey, "seq", sibling)

    def share_body(sc, dq, dk, dv, wq, wk, wv, inv, *refs):
        xs, (own, dot_own, *sends), total = refs[:head_count], refs[head_count:-1], refs[-1]
        total[...] = (
            mm(dq[...], wq[...], NT) + mm(dk[...], wk[...], NT) + mm(dv[...], wv[...], NT)
        ).astype(BF16)
        dot = None
        for p, x in enumerate(xs):
            part = total[:, pl.ds(pl.multiple_of(sc[2 + p], 128), width)]
            if p == 0:
                own[...] = part
            else:
                sends[p - 1][0:tok, :] = part
            term = jnp.sum(part.astype(F32) * x[...].astype(F32), axis=1, keepdims=True)
            dot = term if dot is None else dot + term
        dot = dot * inv[:, 0:1]
        dot_own[...] = jnp.broadcast_to(dot, dot_own.shape)
        high = col_to_row(dot, tok)
        high_wide = high.astype(BF16).astype(F32)
        low_wide = high - high_wide
        row = lax.broadcasted_iota(jnp.int32, (PAD, tok), 0)
        both = jnp.where(row == 0, high_wide, jnp.where(row == 1, low_wide, 0.0)).astype(BF16)
        for s in sends:
            s[tok : tok + PAD, :] = jnp.zeros((PAD, width), BF16)
            s[tok : tok + PAD, 0:tok] = both

    outs = call(
        "share",
        share_body,
        [((tok, width), BF16), ((tok, 128), F32)] + [((tok + PAD, width), BF16)] * (head_count - 1),
        scalars,
        dquery,
        dkey,
        dvalue,
        query_weight,
        key_weight,
        value_weight,
        inv_rms,
        x_own,
        *x_others,
        scratch=[pltpu.VMEM((tok, full), BF16)],
    )
    share_own, dot_own = outs[:2]
    shares = [
        lax.ppermute(o, "head", [(j, (j + p) % head_count) for j in range(head_count)])
        for p, o in enumerate(outs[2:], 1)
    ]

    keep_v, got_v = weight_term("weight_v", dvalue, dvalue_sib)
    keep_k, got_k = weight_term("weight_k", dkey, dkey_sib)
    own_q, blocks_q = rows_term("rows_q", keep_q, got_q)
    own_v, blocks_v = rows_term("rows_v", keep_v, got_v)

    def second_body(sc, x, inv, gpass, own, dot_own, *refs):
        shares, out = refs[:-1], refs[-1]
        total, dot = own[...].astype(F32), dot_own[:, 0:1]
        for s in shares:
            total = total + s[0:tok, :].astype(F32)
            numbers = s[tok : tok + PAD, 0:tok].astype(F32)
            dot = dot + row_to_col(numbers[0:1, :] + numbers[1:2, :], tok)
        norm = x[...].astype(F32) * inv[:, 0:1]
        out[...] = (
            gpass[...].astype(F32) + inv[:, 0:1] * (total - norm * (dot * (1.0 / full)))
        ).astype(BF16)

    (grad_second,) = call(
        "second",
        second_body,
        [((tok, width), BF16)],
        scalars,
        x_own,
        inv_rms,
        grad_pass[0],
        share_own,
        dot_own,
        *shares,
    )
    own_k, blocks_k = rows_term("rows_k", keep_k, got_k)

    return (
        first_in[None],
        grad_second[None],
        final_term(own_q, blocks_q),
        final_term(own_k, blocks_k),
        final_term(own_v, blocks_v),
    )


def solution(mesh):
    placed = (
        P("dp", "seq", "head"),
        P("dp", "seq", "head"),
        P("dp", "seq", "head"),
        P("dp", "seq", "head"),
        P(None, "head"),
        P(None, "head"),
        P(None, "head"),
        P("head", None, None),
        P("dp", "seq"),
    )
    return jax.shard_map(
        shards,
        mesh=mesh,
        in_specs=placed,
        out_specs=(
            P("dp", "seq", "head"),
            P("dp", "seq", "head"),
            P(("seq", "dp"), "head"),
            P(("seq", "dp"), "head"),
            P(("seq", "dp"), "head"),
        ),
        check_vma=False,
    )
```

```python
import jax
import jax.numpy as jnp
from jax import lax
from jax.experimental import pallas as pl
from jax.experimental.pallas import tpu as pltpu
from jax.sharding import PartitionSpec as P

EPSILON = 1e-06
F32 = jnp.float32
BF16 = jnp.bfloat16
VMEM_LIMIT = 16 * 1024 * 1024
PAD = 16


NN = (((1,), (0,)), ((), ()))
NT = (((1,), (1,)), ((), ()))
TN = (((0,), (0,)), ((), ()))


def mm(a, b, dims=NN):
    return lax.dot_general(a, b, dims, preferred_element_type=F32)


def call(body, outs, *arrays, flops=1e7, scratch=(), after=()):
    specs = [pl.BlockSpec(memory_space=pltpu.VMEM) for _ in arrays]
    specs += [pl.BlockSpec(memory_space=pl.ANY) for _ in after]
    count = len(arrays)

    def run(*refs):
        body(*refs[:count], *refs[count + len(after) :])

    return pl.pallas_call(
        run,
        out_shape=[jax.ShapeDtypeStruct(s, d) for s, d in outs],
        in_specs=specs,
        out_specs=[pl.BlockSpec(memory_space=pltpu.VMEM) for _ in outs],
        scratch_shapes=list(scratch),
        cost_estimate=pl.CostEstimate(
            flops=int(flops),
            transcendentals=0,
            bytes_accessed=sum(a.size * a.dtype.itemsize for a in arrays),
        ),
        compiler_params=pltpu.CompilerParams(vmem_limit_bytes=VMEM_LIMIT),
    )(*arrays, *after)


def features(projected, directions, head_dim, count):
    mixing = mm(projected, directions)
    wide = projected.astype(F32)
    squares = jnp.sum(wide * wide, axis=1, keepdims=True)
    exponent = mixing * (1.0 / head_dim**0.25) - squares * (1.0 / (2.0 * head_dim**0.5))
    return (jnp.exp(exponent) * (1.0 / count**0.5)).astype(BF16)


def features_back(dfeature, feature, projected, directions, head_dim):
    dexponent = dfeature * feature.astype(F32)
    back = mm(dexponent.astype(BF16), directions, NT)
    totals = jnp.sum(dexponent, axis=1, keepdims=True)
    result = back * (1.0 / head_dim**0.25) - projected.astype(F32) * (totals * (1.0 / head_dim**0.5))
    return result.astype(BF16)


def eye(n):
    return lax.broadcasted_iota(jnp.int32, (n, n), 0) == lax.broadcasted_iota(jnp.int32, (n, n), 1)


def row_to_col(row, n):
    return jnp.sum(jnp.where(eye(n), row, 0.0), axis=1, keepdims=True)


def col_to_row(col, n):
    return jnp.sum(jnp.where(eye(n), col, 0.0), axis=0, keepdims=True)


def pairs_allowed(id_col, id_row):
    n = id_row.shape[1]
    causal = lax.broadcasted_iota(jnp.int32, (n, n), 0) >= lax.broadcasted_iota(jnp.int32, (n, n), 1)
    return (id_col == id_row) & causal


def merged(refs, wanted, rows):
    total = None
    for ref in refs:
        number = ref[rows : rows + PAD, :].astype(F32)[0:1, 0:1]
        part = ref[0:rows, :].astype(F32) * (number == wanted).astype(F32)
        total = part if total is None else total + part
    return total.astype(BF16)


def shards(
    passthrough,
    mixed_out,
    grad_mixed,
    grad_pass,
    query_weight,
    key_weight,
    value_weight,
    random_features,
    document_ids,
):
    count_ctx, tok, width = passthrough.shape
    heads, head_dim, feats = random_features.shape
    assert count_ctx == 1 and heads * head_dim == width and tok <= width
    seq_count, head_count, dp_count = (lax.axis_size(a) for a in ("seq", "head", "dp"))
    full = width * head_count
    pair_count = seq_count // 2
    assert seq_count % 2 == 0 and pair_count & (pair_count - 1) == 0
    total_rows = count_ctx * tok * seq_count * dp_count
    grad_scale = 1.0 / total_rows**0.5
    reach = max(1, -(-(seq_count * tok // 4 - 1) // tok))
    srows = heads * feats

    x_own = passthrough[0]
    x_others = [
        lax.ppermute(x_own, "head", [(j, (j - p) % head_count) for j in range(head_count)])
        for p in range(1, head_count)
    ]

    def block_start(p):
        return pl.multiple_of(lax.rem(lax.axis_index("head") + p, head_count) * width, width)

    def hsl(h):
        return slice(h * head_dim, (h + 1) * head_dim)

    def fsl(h):
        return slice(h * feats, (h + 1) * feats)

    fetched = (query_weight, key_weight, value_weight, random_features)

    def fetch_body(*refs):
        sources, targets, sem = refs[:4], refs[4:8], refs[8]
        copies = [
            pltpu.make_async_copy(a, b, sem.at[i]) for i, (a, b) in enumerate(zip(sources, targets))
        ]
        for c in copies:
            c.start()
        for c in copies:
            c.wait()

    fetch = pl.pallas_call(
        fetch_body,
        name="fetch",
        out_shape=[jax.ShapeDtypeStruct(a.shape, a.dtype) for a in fetched],
        in_specs=[pl.BlockSpec(memory_space=pltpu.HBM)] * 4,
        out_specs=[pl.BlockSpec(memory_space=pltpu.VMEM)] * 4,
        scratch_shapes=[pltpu.SemaphoreType.DMA((4,))],
        cost_estimate=pl.CostEstimate(flops=10**7, transcendentals=0, bytes_accessed=10**6),
        compiler_params=pltpu.CompilerParams(vmem_limit_bytes=VMEM_LIMIT),
    )
    query_weight, key_weight, value_weight, random_features = fetch(*fetched)

    def keys_body(ids, *refs):
        xs, (wk, wv, rf) = refs[:head_count], refs[head_count : head_count + 3]
        normed, inv_out, key, value, feat_key, tail, id_out = refs[head_count + 3 :]
        squares = None
        for x in xs:
            wide = x[...].astype(F32)
            part = jnp.sum(wide * wide, axis=1, keepdims=True)
            squares = part if squares is None else squares + part
        inv = lax.rsqrt(squares * (1.0 / full) + EPSILON)
        inv_out[...] = jnp.broadcast_to(inv, inv_out.shape)
        for p, x in enumerate(xs):
            normed[:, pl.ds(block_start(p), width)] = (x[...].astype(F32) * inv).astype(BF16)
        id_row = ids[...].astype(F32)
        id_col = row_to_col(id_row, tok)
        id_out[...] = jnp.broadcast_to(id_col, id_out.shape)
        n = normed[...]
        key[...] = mm(n, wk[...]).astype(BF16)
        value[...] = mm(n, wv[...]).astype(BF16)
        last = id_row[:, tok - 1 : tok]
        on = id_col == last
        for h in range(heads):
            feat = features(key[:, hsl(h)], rf[h], head_dim, feats)
            feat_key[:, fsl(h)] = feat
            masked = jnp.where(on, feat.astype(F32), 0.0).astype(BF16)
            tail[fsl(h), :] = mm(masked, value[:, hsl(h)], TN).astype(BF16)
        tail[srows : srows + PAD, :] = jnp.broadcast_to(last, (PAD, head_dim)).astype(BF16)

    normed, inv_rms, key, value, feat_key, tail, id_col = call(
        keys_body,
        [
            ((tok, full), BF16),
            ((tok, 128), F32),
            ((tok, width), BF16),
            ((tok, width), BF16),
            ((tok, srows), BF16),
            ((srows + PAD, head_dim), BF16),
            ((tok, 128), F32),
        ],
        document_ids,
        x_own,
        *x_others,
        key_weight,
        value_weight,
        random_features,
    )

    def shifted(state, sign):
        return [
            lax.ppermute(
                state,
                "seq",
                [(j, j + sign * k) for j in range(seq_count) if 0 <= j + sign * k < seq_count],
            )
            for k in range(1, reach + 1)
        ]

    earlier = shifted(tail, 1)

    def queries_body(ids, idc, normed, wq, rf, feat_key, value, query, feat_query, pair, local):
        query[...] = mm(normed[...], wq[...]).astype(BF16)
        allowed = pairs_allowed(idc[:, 0:1], ids[...].astype(F32))
        for h in range(heads):
            feat = features(query[:, hsl(h)], rf[h], head_dim, feats)
            feat_query[:, fsl(h)] = feat
            scores = mm(feat, feat_key[:, fsl(h)], NT)
            weights = jnp.where(allowed, scores, 0.0).astype(BF16)
            pair[h] = weights
            local[:, hsl(h)] = mm(weights, value[:, hsl(h)])

    query, feat_query, pair, attn_local = call(
        queries_body,
        [
            ((tok, width), BF16),
            ((tok, srows), BF16),
            ((heads, tok, tok), BF16),
            ((tok, width), F32),
        ],
        document_ids,
        id_col,
        normed,
        query_weight,
        random_features,
        feat_key,
        value,
    )

    blocks = pair_count * dp_count
    block_rows = full // (2 * blocks)

    def turned_body(normed, mine, theirs, held):
        seq_at, dp_at = lax.axis_index("seq"), lax.axis_index("dp")
        pair_at, core_at = lax.div(seq_at, 2), lax.rem(seq_at, 2)
        turned = normed[...].astype(F32).T
        for b in range(2 * blocks):
            held[b] = turned[b * block_rows : (b + 1) * block_rows, :].astype(BF16)
        for p in range(dp_count):
            for k in range(pair_count):
                pair = lax.bitwise_xor(pair_at, k) * 2
                column = lax.rem(dp_at + p, dp_count)
                mine[p * pair_count + k] = held[(pair + core_at) * dp_count + column]
                theirs[p * pair_count + k] = held[(pair + 1 - core_at) * dp_count + column]

    shape3 = (blocks, block_rows, tok)
    mine_t, theirs_t = call(
        turned_body,
        [(shape3, BF16), (shape3, BF16)],
        normed,
        after=[query],
        scratch=[pltpu.VMEM((2 * blocks, block_rows, tok), BF16)],
    )
    sibling = [(j, j ^ 1) for j in range(seq_count)]
    sibling_t = lax.ppermute(theirs_t, "seq", sibling)
    mine_t = mine_t.reshape(blocks * block_rows, tok)
    sibling_t = sibling_t.reshape(blocks * block_rows, tok)

    def attend_body(idc, feat_query, local, mixed, gmixed, *refs):
        states, (first_in, grad_attn, head_state, state) = refs[:reach], refs[reach:]
        first = idc[0:1, 0:1]
        state[...] = merged(states, first, srows)
        on = idc[:, 0:1] == first
        for h in range(heads):
            fq = feat_query[:, fsl(h)]
            carried = mm(fq, state[fsl(h), :])
            attn = local[:, hsl(h)] + jnp.where(on, carried, 0.0)
            inv = lax.rsqrt(jnp.mean(attn * attn, axis=1, keepdims=True) + EPSILON)
            act = attn * inv
            first_in[:, hsl(h)] = (mixed[:, hsl(h)].astype(F32) - act).astype(BF16)
            g = gmixed[:, hsl(h)].astype(F32)
            ga = (inv * (g - act * jnp.mean(g * act, axis=1, keepdims=True))).astype(BF16)
            grad_attn[:, hsl(h)] = ga
            masked = jnp.where(on, fq.astype(F32), 0.0).astype(BF16)
            head_state[fsl(h), :] = mm(masked, ga, TN).astype(BF16)
        head_state[srows : srows + PAD, :] = jnp.broadcast_to(first, (PAD, head_dim)).astype(BF16)

    first_in, grad_attn, head_state, state_in = call(
        attend_body,
        [
            ((tok, width), BF16),
            ((tok, width), BF16),
            ((srows + PAD, head_dim), BF16),
            ((srows, head_dim), BF16),
        ],
        id_col,
        feat_query,
        attn_local,
        mixed_out[0],
        grad_mixed[0],
        *earlier,
        after=[theirs_t],
    )

    later = shifted(head_state, -1)

    def dquery_body(ids, idc, grad_attn, value, feat_key, feat_query, query, rf, state, dquery, dpair):
        first = idc[0:1, 0:1]
        on = idc[:, 0:1] == first
        allowed = pairs_allowed(idc[:, 0:1], ids[...].astype(F32))
        for h in range(heads):
            ga = grad_attn[:, hsl(h)]
            dscores = mm(ga, value[:, hsl(h)], NT)
            dp = jnp.where(allowed, dscores, 0.0).astype(BF16)
            dpair[h] = dp
            dfeat = mm(dp, feat_key[:, fsl(h)]) + jnp.where(on, mm(ga, state[fsl(h), :], NT), 0.0)
            dquery[:, hsl(h)] = features_back(
                dfeat, feat_query[:, fsl(h)], query[:, hsl(h)], rf[h], head_dim
            )

    dquery, dpair = call(
        dquery_body,
        [((tok, width), BF16), ((heads, tok, tok), BF16)],
        document_ids,
        id_col,
        grad_attn,
        value,
        feat_key,
        feat_query,
        query,
        random_features,
        state_in,
    )
    dquery_sib = lax.ppermute(dquery, "seq", sibling)

    def local_body(dpair, pair, feat_query, grad_attn, dfeat, dvalue):
        for h in range(heads):
            dfeat[:, fsl(h)] = mm(dpair[h], feat_query[:, fsl(h)], TN)
            dvalue[:, hsl(h)] = mm(pair[h], grad_attn[:, hsl(h)], TN)

    dfeat_local, dvalue_local = call(
        local_body,
        [((tok, srows), F32), ((tok, width), F32)],
        dpair,
        pair,
        feat_query,
        grad_attn,
        after=[dquery],
    )

    rows_send = pair_count * block_rows

    def weight_body(mine, sib, d, dsib, keep, *sends):
        for p in range(dp_count):
            at = slice(p * rows_send, (p + 1) * rows_send)
            part = (mm(mine[at, :], d[...]) + mm(sib[at, :], dsib[...])) * grad_scale
            if p == 0:
                keep[...] = part
            else:
                sends[p - 1][...] = part.astype(BF16)

    def weight_term(d, dsib, *after):
        outs = call(
            weight_body,
            [((rows_send, width), F32)] + [((rows_send, width), BF16)] * (dp_count - 1),
                mine_t,
            sibling_t,
            d,
            dsib,
            after=after,
        )
        return outs[0], outs[1], [
            lax.ppermute(o, "dp", [(j, (j + p) % dp_count) for j in range(dp_count)])
            for p, o in enumerate(outs[1:], 1)
        ]

    def rows_body(keep, *refs):
        got, (own, *sends) = refs[: dp_count - 1], refs[dp_count - 1 :]
        for k in range(pair_count):
            at = slice(k * block_rows, (k + 1) * block_rows)
            total = keep[at, :]
            for g in got:
                total = total + g[at, :].astype(F32)
            if k == 0:
                own[...] = total
            else:
                sends[k - 1][...] = total.astype(BF16)

    def rows_term(keep, got, *after):
        outs = call(
            rows_body,
            [((block_rows, width), F32)] + [((block_rows, width), BF16)] * (pair_count - 1),
                keep,
            *got,
            after=after,
        )
        return outs[0], [
            lax.ppermute(o, "seq", [(j, ((j // 2) ^ k) * 2 + j % 2) for j in range(seq_count)])
            for k, o in enumerate(outs[1:], 1)
        ]

    def final_term(own, got):
        for g in got:
            own = own + g.astype(F32)
        return own

    keep_q, send_q, got_q = weight_term(dquery, dquery_sib, dvalue_local)

    def dvalue_body(idc, dvalue_local, feat_key, *refs):
        states, (dvalue, state) = refs[:reach], refs[reach:]
        last = idc[tok - 1 : tok, 0:1]
        state[...] = merged(states, last, srows)
        on = idc[:, 0:1] == last
        for h in range(heads):
            carried = mm(feat_key[:, fsl(h)], state[fsl(h), :])
            dvalue[:, hsl(h)] = (dvalue_local[:, hsl(h)] + jnp.where(on, carried, 0.0)).astype(BF16)

    dvalue, state_later = call(
        dvalue_body,
        [((tok, width), BF16), ((srows, head_dim), BF16)],
        id_col,
        dvalue_local,
        feat_key,
        *later,
        after=[send_q],
    )
    dvalue_sib = lax.ppermute(dvalue, "seq", sibling)

    def dkey_body(idc, dfeat_local, feat_key, value, key, rf, state, dkey):
        on = idc[:, 0:1] == idc[tok - 1 : tok, 0:1]
        for h in range(heads):
            carried = mm(value[:, hsl(h)], state[fsl(h), :], NT)
            dfeat = dfeat_local[:, fsl(h)] + jnp.where(on, carried, 0.0)
            dkey[:, hsl(h)] = features_back(
                dfeat, feat_key[:, fsl(h)], key[:, hsl(h)], rf[h], head_dim
            )

    (dkey,) = call(
        dkey_body,
        [((tok, width), BF16)],
        id_col,
        dfeat_local,
        feat_key,
        value,
        key,
        random_features,
        state_later,
    )
    dkey_sib = lax.ppermute(dkey, "seq", sibling)
    own_q, blocks_q = rows_term(keep_q, got_q, dkey)
    keep_v, send_v, got_v = weight_term(dvalue, dvalue_sib, own_q)
    keep_k, send_k, got_k = weight_term(dkey, dkey_sib, send_v)

    def share_body(dq, dk, dv, wq, wk, wv, inv, *refs):
        xs, (own, dot_own, *sends), total = refs[:head_count], refs[head_count:-1], refs[-1]
        total[...] = (
            mm(dq[...], wq[...], NT) + mm(dk[...], wk[...], NT) + mm(dv[...], wv[...], NT)
        ).astype(BF16)
        dot = None
        for p, x in enumerate(xs):
            part = total[:, pl.ds(block_start(p), width)]
            if p == 0:
                own[...] = part
            else:
                sends[p - 1][0:tok, :] = part
            term = jnp.sum(part.astype(F32) * x[...].astype(F32), axis=1, keepdims=True)
            dot = term if dot is None else dot + term
        dot = dot * inv[:, 0:1]
        dot_own[...] = jnp.broadcast_to(dot, dot_own.shape)
        high = col_to_row(dot, tok)
        high_wide = high.astype(BF16).astype(F32)
        low_wide = high - high_wide
        row = lax.broadcasted_iota(jnp.int32, (PAD, tok), 0)
        both = jnp.where(row == 0, high_wide, jnp.where(row == 1, low_wide, 0.0)).astype(BF16)
        for s in sends:
            s[tok : tok + PAD, :] = jnp.zeros((PAD, width), BF16)
            s[tok : tok + PAD, 0:tok] = both

    outs = call(
        share_body,
        [((tok, width), BF16), ((tok, 128), F32)] + [((tok + PAD, width), BF16)] * (head_count - 1),
        dquery,
        dkey,
        dvalue,
        query_weight,
        key_weight,
        value_weight,
        inv_rms,
        x_own,
        *x_others,
        scratch=[pltpu.VMEM((tok, full), BF16)],
        after=[send_k],
    )
    share_own, dot_own = outs[:2]
    shares = [
        lax.ppermute(o, "head", [(j, (j + p) % head_count) for j in range(head_count)])
        for p, o in enumerate(outs[2:], 1)
    ]

    own_v, blocks_v = rows_term(keep_v, got_v, share_own)

    def second_body(x, inv, gpass, own, dot_own, *refs):
        shares, (out, done) = refs[:-2], refs[-2:]
        done[...] = jnp.zeros_like(done)
        total, dot = own[...].astype(F32), dot_own[:, 0:1]
        for s in shares:
            total = total + s[0:tok, :].astype(F32)
            numbers = s[tok : tok + PAD, 0:tok].astype(F32)
            dot = dot + row_to_col(numbers[0:1, :] + numbers[1:2, :], tok)
        norm = x[...].astype(F32) * inv[:, 0:1]
        out[...] = (
            gpass[...].astype(F32) + inv[:, 0:1] * (total - norm * (dot * (1.0 / full)))
        ).astype(BF16)

    grad_second, second_done = call(
        second_body,
        [((tok, width), BF16), ((8, 128), F32)],
        x_own,
        inv_rms,
        grad_pass[0],
        share_own,
        dot_own,
        *shares,
        after=[own_v],
    )
    own_k, blocks_k = rows_term(keep_k, got_k, second_done)

    return (
        first_in[None],
        grad_second[None],
        final_term(own_q, blocks_q),
        final_term(own_k, blocks_k),
        final_term(own_v, blocks_v),
    )


def solution(mesh):
    placed = (
        P("dp", "seq", "head"),
        P("dp", "seq", "head"),
        P("dp", "seq", "head"),
        P("dp", "seq", "head"),
        P(None, "head"),
        P(None, "head"),
        P(None, "head"),
        P("head", None, None),
        P("dp", "seq"),
    )
    return jax.shard_map(
        shards,
        mesh=mesh,
        in_specs=placed,
        out_specs=(
            P("dp", "seq", "head"),
            P("dp", "seq", "head"),
            P(("seq", "dp"), "head"),
            P(("seq", "dp"), "head"),
            P(("seq", "dp"), "head"),
        ),
        check_vma=False,
    )
```
